32 devices in a mesh: group: 2 (over y), expert: 4 (over z), tensor: 2 (over core), section: 2 (over x).
Axes of the slice: x: 2, y: 2, z: 4, core: 2. Of those that a mesh axis runs over, the one named last changes fastest.
Arguments:
- tokens: bfloat16 [32, 2048], P(('group', 'expert')), parts along dimension 0, may hold values from -10 to 10
- lengths: int32 [32], P(('group', 'expert')), parts along dimension 0, may hold values from 1 to 256, as said below
- routes: int32 [2, 32, 2], P('section', ('group', 'expert')), parts along dimension 1, may hold values from 0 to 3, all different within a row
- attn_gain: float32 [2, 2048], P('section'), may hold values from 0.4 to 1.6
- w_qkv: bfloat16 [2, 2, 2048, 1536], P('section', 'tensor', None, 'expert'), may hold values from -0.5 to 0.5
- w_out: bfloat16 [2, 2048, 2048], P('section', 'tensor', 'expert'), may hold values from -0.125 to 0.125
- moe_gain: float32 [2, 2048], P('section'), may hold values from 0.4 to 1.6
- router: bfloat16 [2, 2048, 4], P('section'), may hold values from -0.125 to 0.125
- w_up: bfloat16 [2, 2048, 28672], P('section', None, ('expert', 'tensor')), may hold values from -0.125 to 0.125
- w_down: bfloat16 [2, 28672, 2048], P('section', ('expert', 'tensor')), may hold values from -0.0625 to 0.0625
- k_codes: int32 [2, 32, 16, 512], P('section', ('group', 'expert'), None, 'tensor'), parts along dimension 1, may hold values from -2147483648 to 2147483646
- k_scale: bfloat16 [2, 32, 8, 512], P('section', ('group', 'expert'), None, 'tensor'), parts along dimension 1, may hold values from 0.25 to 1
- k_zero: bfloat16 [2, 32, 8, 512], P('section', ('group', 'expert'), None, 'tensor'), parts along dimension 1, may hold values from -4 to 4
- v_codes: int32 [2, 32, 16, 512], P('section', ('group', 'expert'), None, 'tensor'), parts along dimension 1, may hold values from -2147483648 to 2147483646
- v_scale: bfloat16 [2, 32, 16, 256], P('section', ('group', 'expert'), 'tensor'), parts along dimension 1, may hold values from 0.25 to 1
- v_zero: bfloat16 [2, 32, 16, 256], P('section', ('group', 'expert'), 'tensor'), parts along dimension 1, may hold values from -4 to 4
Outputs:
- layer_outputs: bfloat16 [2, 32, 2048], P('section', ('group', 'expert')), parts along dimension 1
The draws below stay inside these ranges and needn't reach their ends.
There are 2 independent parts, one for each index of `group`. The reference program is written for one: setup_inputs(seed, part) draws one part's arguments, and reference() takes and returns one part's arrays. A program takes and returns all parts, laid end to end along the dimension named above; an argument that names none is the same for every part. Nothing has to cross between parts.
Inputs may be any that keep to these rules, and one draw needn't show every extreme that they name: Each sequence has cached positions 0 to lengths - 1 and its new token stands at position lengths; some sequence has all 256. `routes`: the two experts of a token differ. `k_codes`: word w holds the codes of positions 16 * w to 16 * w + 15, position 16 * w + i in bits 2 * i and 2 * i + 1. `v_codes`: packed as the key codes.
All inputs are finite; a program needn't handle non-finite values.
Results may differ from the reference program's by a relative error of at most 0.015.
Values may be sent and summed in bfloat16 or wider, within the bound.
No kernel may reach another device: no remote copies, remote signals or barrier semaphores. Data moves between devices by JAX's collectives and lax.ppermute only.
A program may use at most 64 MiB of HBM per device.

```python
import math
import jax
import jax.numpy as jnp
from jax import lax

D = 2048
HEADS = 16
KV_HEADS = 4
HEAD_DIM = 128
FF = 7168
EXPERTS = 4
CTX = 256
PACK = 16
KGROUP = 32
VGROUP = 32
HALVES = 2
QKV_COLS = 1536
KVC = 512
SEQS = 16
LAYERS = 2
N_EXPERT = 4
N_TENSOR = 2


def draw_lengths(key, part):
    first_key, second_key = jax.random.split(jax.random.fold_in(key, 11))
    drawn = jax.random.randint(first_key, (SEQS,), 1, CTX + 1, dtype=jnp.int32)
    chosen = jax.random.randint(second_key, (), 0, SEQS, dtype=jnp.int32)
    return jnp.where(jnp.arange(SEQS, dtype=jnp.int32) == chosen, CTX, drawn).astype(jnp.int32)


def draw_tokens(key, part):
    base_key, pick_key, noise_key = jax.random.split(jax.random.fold_in(key, 21), 3)
    return jnp.clip(jax.random.normal(base_key, (SEQS, D), jnp.float32), -6.0, 6.0).astype(jnp.bfloat16)


def draw_w_qkv(key, part):
    normal_draw = jax.random.normal(jax.random.fold_in(key, 31), (LAYERS, HALVES, D, QKV_COLS), jnp.float32)
    scaled = jnp.clip(normal_draw / math.sqrt(D), -0.45, 0.45)
    return scaled.astype(jnp.bfloat16)


def draw_k_zero(key, part):
    table_shape = (LAYERS, SEQS, CTX // KGROUP, KVC)
    zero_key = jax.random.fold_in(key, 41)
    return jnp.clip(jax.random.normal(zero_key, table_shape, jnp.float32), -4.0, 4.0).astype(jnp.bfloat16)


def set_ends(result, key, low, largest):
    index_at = [jax.random.randint(jax.random.fold_in(key, axis), (), 0, length) for axis, length in enumerate(result.shape)]
    longest = result.shape.index(max(result.shape))
    beside = index_at[:longest] + [(index_at[longest] + 1) % result.shape[longest]] + index_at[longest + 1:]
    return result.at[tuple(index_at)].set(low).at[tuple(beside)].set(largest)


def shard_levels(key, shape, cuts, low, largest):
    level = 1.0
    for position, parts in cuts:
        heights = jax.random.uniform(jax.random.fold_in(jax.random.fold_in(key, 6), position), (parts,), jnp.float32, low / len(cuts), largest / len(cuts))
        level = level * jnp.repeat(jnp.exp(heights), shape[position] // parts).reshape((-1,) + (1,) * (len(shape) - 1 - position))
    return level


def different_ones(key, rows, number_of, top, lift):
    ranking = jax.random.permutation(jax.random.fold_in(key, 1), number_of)
    favour = ranking
    for power in range(3):
        favour = favour * favour // number_of
    favour = favour * lift // number_of
    lots = jax.random.randint(jax.random.fold_in(key, 2), (rows, number_of), 0, 4096) + favour
    fixed_rows = jax.random.permutation(jax.random.fold_in(key, 3), rows)[jnp.arange(number_of) % rows]
    lots = jnp.where(jnp.arange(rows)[:, None] == fixed_rows[None, :], 1 << 14, lots)
    score = lots * number_of + jnp.arange(number_of)
    return lax.top_k(score.astype(jnp.int32), top)[1].astype(jnp.int32)


def normal_values(stream_key, shape, scale, limit, cuts=(), held_as=jnp.bfloat16):
    values = scale * jax.random.normal(stream_key, shape, jnp.float32)
    if cuts:
        values = values * shard_levels(stream_key, shape, cuts, -0.22, 0.18)
    return jnp.clip(values, -limit, limit).astype(held_as)


def setup_inputs(seed: int = 0, part: int = 0) -> dict:
    key_of = jax.random.split(jax.random.key(seed), 17)
    own_keys = jax.random.split(jax.random.fold_in(key_of[16], part), 17)
    tokens = draw_tokens(jax.random.fold_in(jax.random.fold_in(key_of[16], part), 71), part)
    lengths = draw_lengths(jax.random.fold_in(jax.random.fold_in(key_of[16], part), 71), part)
    routes = different_ones(own_keys[2], LAYERS * SEQS, EXPERTS, 2, 8192).reshape((LAYERS, SEQS, 2))
    attn_gain = jnp.clip(1.0 + 0.12 * jax.random.normal(key_of[3], (LAYERS, D), jnp.float32), 0.4, 1.6)
    w_qkv = draw_w_qkv(jax.random.fold_in(key_of[16], 71), part)
    w_out = normal_values(key_of[5], (LAYERS, HEADS * HEAD_DIM, D), (HEADS * HEAD_DIM) ** -0.5, 0.125, ((0, 2), (1, 2), (2, 4)))
    moe_gain = jnp.clip(1.0 + 0.12 * jax.random.normal(key_of[6], (LAYERS, D), jnp.float32), 0.4, 1.6)
    router = normal_values(key_of[7], (LAYERS, D, EXPERTS), D ** -0.5, 0.125, ((0, 2),))
    w_up = normal_values(key_of[8], (LAYERS, D, EXPERTS * FF), D ** -0.5, 0.125, ((0, 2), (2, 8)))
    w_down = normal_values(key_of[9], (LAYERS, EXPERTS * FF, D), FF ** -0.5, 0.0625, ((0, 2), (1, 8)))
    k_codes = set_ends(jax.random.randint(own_keys[10], (LAYERS, SEQS, CTX // PACK, KVC), -2147483648, 2147483647), jax.random.fold_in(own_keys[10], 1), -2147483648, 2147483646).astype(jnp.int32)
    k_scale = jnp.clip(jnp.exp(math.log(1.0) - 1.3862944 * jax.random.uniform(own_keys[11], (LAYERS, SEQS, CTX // KGROUP, KVC), jnp.float32) ** shard_levels(own_keys[11], (LAYERS, SEQS, CTX // KGROUP, KVC), ((0, 2), (1, 4), (3, 2)), -0.2, 0.2)), 0.25, 1.0).astype(jnp.bfloat16)
    k_zero = draw_k_zero(jax.random.fold_in(jax.random.fold_in(key_of[16], part), 71), part)
    v_codes = set_ends(jax.random.randint(own_keys[13], (LAYERS, SEQS, CTX // PACK, KVC), -2147483648, 2147483647), jax.random.fold_in(own_keys[13], 1), -2147483648, 2147483646).astype(jnp.int32)
    v_scale = jnp.clip(jnp.exp(math.log(1.0) - 1.3862944 * jax.random.uniform(own_keys[14], (LAYERS, SEQS, KVC // VGROUP, CTX), jnp.float32) ** shard_levels(own_keys[14], (LAYERS, SEQS, KVC // VGROUP, CTX), ((0, 2), (1, 4), (2, 2)), -0.2, 0.2)), 0.25, 1.0).astype(jnp.bfloat16)
    v_zero = normal_values(own_keys[15], (LAYERS, SEQS, KVC // VGROUP, CTX), 1.0, 4.0, ((0, 2), (1, 4), (2, 2)))
    return {"tokens": tokens, "lengths": lengths, "routes": routes, "attn_gain": attn_gain, "w_qkv": w_qkv, "w_out": w_out, "moe_gain": moe_gain, "router": router, "w_up": w_up, "w_down": w_down, "k_codes": k_codes, "k_scale": k_scale, "k_zero": k_zero, "v_codes": v_codes, "v_scale": v_scale, "v_zero": v_zero}


rope_base = 1000000.0
norm_eps = 1e-05

def rms_scale(values, gain_row):
    widened = values.astype(jnp.float32)
    return widened * lax.rsqrt(lax.optimization_barrier(jnp.mean(widened * widened, axis=-1, keepdims=True)) + norm_eps) * gain_row

def rotate(vector, angles):
    half_width = vector.shape[-1] // 2
    front_half = vector[..., :half_width]
    back_half = vector[..., half_width:]
    cosine_val = jnp.cos(angles)
    sine_val = jnp.sin(angles)
    return jnp.concatenate([front_half * cosine_val - back_half * sine_val, back_half * cosine_val + front_half * sine_val], axis=-1)

def unpack(packed):
    shifts = 2 * jnp.arange(16, dtype=jnp.int32)
    code_vals = jnp.bitwise_and(jnp.right_shift(packed[:, :, None, :], shifts[None, None, :, None]), 3)
    return code_vals.reshape(packed.shape[0], packed.shape[1] * 16, packed.shape[2])

def dequant_keys(packed, scales, zero_table):
    code_vals = unpack(packed).astype(jnp.float32)
    seq_count, positions, channels = code_vals.shape
    grouped = code_vals.reshape(seq_count, scales.shape[1], positions // scales.shape[1], channels)
    dequant = grouped * scales.astype(jnp.float32)[:, :, None, :] + zero_table.astype(jnp.float32)[:, :, None, :]
    return dequant.reshape(seq_count, positions, channels).astype(jnp.bfloat16)

def dequant_values(packed, scales, zero_table):
    code_vals = unpack(packed).astype(jnp.float32)
    seq_count, positions, channels = code_vals.shape
    groups = scales.shape[1]
    grouped = code_vals.reshape(seq_count, positions, groups, channels // groups)
    scale_turned = jnp.transpose(scales.astype(jnp.float32), (0, 2, 1))[:, :, :, None]
    zero_turned = jnp.transpose(zero_table.astype(jnp.float32), (0, 2, 1))[:, :, :, None]
    dequant = grouped * scale_turned + zero_turned
    return dequant.reshape(seq_count, positions, channels).astype(jnp.bfloat16)

def attend(queries, own_key, own_value, key_cache, value_cache, seq_lengths):
    scale_root = math.sqrt(queries.shape[-1])
    scores = jnp.einsum('skrd,spkd->skrp', queries.astype(jnp.float32), key_cache.astype(jnp.float32)) / scale_root
    own_score = jnp.einsum('skrd,skd->skr', queries.astype(jnp.float32), own_key.astype(jnp.float32)) / scale_root
    visible = (jnp.arange(key_cache.shape[1], dtype=jnp.int32)[None, :] < seq_lengths[:, None])[:, None, None, :]
    highest = jnp.maximum(lax.optimization_barrier(jnp.max(jnp.where(visible, scores, -1e+30), axis=-1)), own_score)
    exponents = jnp.where(visible, jnp.exp(scores - highest[..., None]), 0.0)
    own_exp = jnp.exp(own_score - highest)
    denominator = lax.optimization_barrier(jnp.sum(exponents, axis=-1)) + own_exp
    probabilities = (exponents / denominator[..., None]).astype(jnp.bfloat16)
    own_prob = (own_exp / denominator).astype(jnp.bfloat16)
    mixture = jnp.einsum('skrp,spkd->skrd', probabilities.astype(jnp.float32), value_cache.astype(jnp.float32))
    mixture = mixture + own_prob.astype(jnp.float32)[..., None] * own_value.astype(jnp.float32)[:, :, None, :]
    return mixture.astype(jnp.bfloat16).reshape(queries.shape[0], -1)

def decode_layer(layer_in, lengths, route, attn_gain, w_qkv, w_out, moe_gain, router, w_up, w_down, k_codes, k_scale, k_zero, v_codes, v_scale, v_zero):
    seq_count = layer_in.shape[0]
    q_local = HEADS // N_TENSOR
    kv_local = KV_HEADS // N_TENSOR
    group_ratio = HEADS // KV_HEADS
    normed = rms_scale(layer_in, attn_gain).astype(jnp.bfloat16)
    half_list = [jnp.dot(normed, w_qkv[half_index], preferred_element_type=jnp.float32).astype(jnp.bfloat16) for half_index in range(N_TENSOR)]
    queries = jnp.concatenate([half_cols[:, :q_local * HEAD_DIM] for half_cols in half_list], axis=1)
    new_keys = jnp.concatenate([half_cols[:, q_local * HEAD_DIM:(q_local + kv_local) * HEAD_DIM] for half_cols in half_list], axis=1)
    new_values = jnp.concatenate([half_cols[:, (q_local + kv_local) * HEAD_DIM:] for half_cols in half_list], axis=1)
    queries = queries.reshape(seq_count, KV_HEADS, group_ratio, HEAD_DIM)
    new_keys = new_keys.reshape(seq_count, KV_HEADS, HEAD_DIM)
    new_values = new_values.reshape(seq_count, KV_HEADS, HEAD_DIM)
    frequency = jnp.power(rope_base, -2.0 * jnp.arange(HEAD_DIM // 2, dtype=jnp.float32) / HEAD_DIM)
    angles = lengths.astype(jnp.float32)[:, None] * frequency[None, :]
    query_rot = rotate(queries.astype(jnp.float32), angles[:, None, None, :]).astype(jnp.bfloat16)
    key_rot = rotate(new_keys.astype(jnp.float32), angles[:, None, :]).astype(jnp.bfloat16)
    key_cache = dequant_keys(k_codes, k_scale, k_zero).reshape(seq_count, CTX, KV_HEADS, HEAD_DIM)
    value_cache = dequant_values(v_codes, v_scale, v_zero).reshape(seq_count, CTX, KV_HEADS, HEAD_DIM)
    attended = attend(query_rot, key_rot, new_values, key_cache, value_cache, lengths)
    out_sum = jnp.dot(attended, w_out, preferred_element_type=jnp.float32)
    hidden = (layer_in.astype(jnp.float32) + out_sum).astype(jnp.bfloat16)
    moe_in = rms_scale(hidden, moe_gain).astype(jnp.bfloat16)
    logits = jnp.dot(moe_in, router, preferred_element_type=jnp.float32)
    chosen = route[:, :, None] == jnp.arange(EXPERTS, dtype=jnp.int32)[None, None, :]
    picked = lax.optimization_barrier(jnp.sum(jnp.where(chosen, logits[:, None, :], 0.0), axis=-1))
    gate_first = 1.0 / (1.0 + jnp.exp(picked[:, 1] - picked[:, 0]))
    gate_second = 1.0 / (1.0 + jnp.exp(picked[:, 0] - picked[:, 1]))
    block_count = N_EXPERT // EXPERTS * N_TENSOR
    block_width = FF // block_count
    moe_out = jnp.zeros((seq_count, D), jnp.float32)
    for expert in range(EXPERTS):
        up_proj = jnp.dot(moe_in, w_up[:, expert * FF:(expert + 1) * FF], preferred_element_type=jnp.float32)
        active = jax.nn.silu(up_proj).astype(jnp.bfloat16)
        pieces = jnp.einsum('snf,nfd->snd', active.reshape(seq_count, block_count, block_width).astype(jnp.float32), w_down[expert * FF:(expert + 1) * FF].reshape(block_count, block_width, D).astype(jnp.float32))
        rounded = lax.optimization_barrier(pieces.astype(jnp.bfloat16))
        summed = lax.optimization_barrier(jnp.sum(rounded.astype(jnp.float32), axis=1))
        weight = jnp.where(route[:, 0] == expert, gate_first, 0.0) + jnp.where(route[:, 1] == expert, gate_second, 0.0)
        moe_out = moe_out + weight[:, None] * summed
    return (hidden.astype(jnp.float32) + moe_out).astype(jnp.bfloat16)

def reference(tokens, lengths, routes, attn_gain, w_qkv, w_out, moe_gain, router, w_up, w_down, k_codes, k_scale, k_zero, v_codes, v_scale, v_zero):
    current = tokens
    layer_list = []
    for layer_index in range(LAYERS):
        current = decode_layer(current, lengths, routes[layer_index], attn_gain[layer_index], w_qkv[layer_index], w_out[layer_index], moe_gain[layer_index], router[layer_index], w_up[layer_index], w_down[layer_index], k_codes[layer_index], k_scale[layer_index], k_zero[layer_index], v_codes[layer_index], v_scale[layer_index], v_zero[layer_index])
        layer_list.append(current)
    return jnp.stack(layer_list)
```

```python
import functools
import math

import jax
import jax.numpy as jnp
from jax import lax
from jax.experimental import pallas as pl
from jax.experimental.pallas import tpu as pltpu
from jax.sharding import PartitionSpec as P

HEAD_DIM = 128
EXPERTS = 4
WORD = 16
rope_base = 1000000.0
norm_eps = 1e-05
FEW = 8
F32 = jnp.float32
BF16 = jnp.bfloat16


def shifted(array, by):
    n = lax.axis_size("expert")
    return lax.ppermute(array, "expert", [(i, (i + by) % n) for i in range(n)])


def arrange(pieces, index, axis):
    n = len(pieces)
    chunks = []
    for j in range(n):
        chunk = pieces[0]
        for k in range(1, n):
            chunk = jnp.where((index - k) % n == j, pieces[k], chunk)
        chunks.append(chunk)
    return jnp.concatenate(chunks, axis=axis)


def gathered(array, axis):
    n = lax.axis_size("expert")
    if n > FEW:
        return lax.all_gather(array, "expert", axis=axis, tiled=True)
    pieces = [array] + [shifted(array, k) for k in range(1, n)]
    return arrange(pieces, lax.axis_index("expert"), axis)


def row_block(array, block, rows):
    return lax.dynamic_slice_in_dim(array, block * rows, rows, 0)


def to_owners(array, rows):
    n = lax.axis_size("expert")
    if n > FEW:
        return lax.all_to_all(array, "expert", split_axis=0, concat_axis=1, tiled=True)
    index = lax.axis_index("expert")
    pieces = [row_block(array, index, rows)]
    for k in range(1, n):
        pieces.append(shifted(row_block(array, (index + k) % n, rows), k))
    return arrange(pieces, index, 1)


def summed_at_owners(own, array, rows):
    n = lax.axis_size("expert")
    index = lax.axis_index("expert")
    if n > FEW:
        got = lax.all_to_all(
            array.reshape(n, rows, -1), "expert", split_axis=0, concat_axis=0, tiled=True
        ).astype(F32)
        return jnp.sum(jnp.where(jnp.arange(n)[:, None, None] == index, own[None], got), axis=0)
    total = own
    for k in range(1, n):
        total = total + shifted(row_block(array, (index + k) % n, rows), k).astype(F32)
    return total


def next_section_sum(array):
    n = lax.axis_size("expert")
    sections = lax.axis_size("section")
    if n > FEW:
        moved = lax.ppermute(array, "section", [(s, s + 1) for s in range(sections - 1)])
        return lax.psum(moved.astype(F32), "expert")
    total = None
    for k in range(n):
        pairs = [
            (e * sections + s, ((e + k) % n) * sections + s + 1)
            for e in range(n)
            for s in range(sections - 1)
        ]
        part = lax.ppermute(array, ("expert", "section"), pairs).astype(F32)
        total = part if total is None else total + part
    return total


def partner(array):
    n = lax.axis_size("tensor")
    return lax.ppermute(array, "tensor", [(i, n - 1 - i) for i in range(n)])


def dot(a, b):
    return jnp.dot(a, b, preferred_element_type=F32)


def dequant_kernel(kc, ks, kz, vc, vs, vz, keys, values):
    seqs, words, channels = kc.shape
    positions = words * WORD
    key_groups = ks.shape[1]
    value_groups = vs.shape[1]
    row = lax.broadcasted_iota(jnp.int32, (positions, positions), 0)
    col = lax.broadcasted_iota(jnp.int32, (positions, positions), 1)
    order = jnp.where(col == (row % words) * WORD + row // words, 1.0, 0.0).astype(BF16)
    group_row = lax.broadcasted_iota(jnp.int32, (value_groups, channels), 0)
    group_col = lax.broadcasted_iota(jnp.int32, (value_groups, channels), 1)
    spread = jnp.where(group_row == group_col // (channels // value_groups), 1.0, 0.0).astype(BF16)
    word_row = lax.broadcasted_iota(jnp.int32, (words, key_groups), 0)
    word_col = lax.broadcasted_iota(jnp.int32, (words, key_groups), 1)
    repeat = jnp.where(word_row // (words // key_groups) == word_col, 1.0, 0.0).astype(BF16)

    def expand(table):
        wide = lax.dot_general(table, spread, (((0,), (0,)), ((), ())), preferred_element_type=F32)
        return dot(order, wide.astype(BF16))

    for s in range(seqs):
        key_scale = dot(repeat, ks[s])
        key_zero = dot(repeat, kz[s])
        value_scale = expand(vs[s])
        value_zero = expand(vz[s])
        for i in range(WORD):
            at = slice(i * words, (i + 1) * words)
            code = ((kc[s] >> (2 * i)) & 3).astype(F32)
            keys[s, at, :] = (code * key_scale + key_zero).astype(BF16)
            code = ((vc[s] >> (2 * i)) & 3).astype(F32)
            values[s, at, :] = (code * value_scale[at] + value_zero[at]).astype(BF16)


def attention_kernel(lengths, heads_in, cosines, sines, keys, values, out):
    seqs, positions, channels = keys.shape
    kv = channels // HEAD_DIM
    queries = out.shape[1]
    ratio = queries // kv
    words = positions // WORD
    place = lax.broadcasted_iota(jnp.int32, (queries, positions), 1)
    place = (place % words) * WORD + place // words
    head = lax.broadcasted_iota(jnp.int32, (queries, HEAD_DIM), 0) // ratio
    wide_head = lax.broadcasted_iota(jnp.int32, (queries, positions), 0) // ratio
    root = math.sqrt(HEAD_DIM)
    for s in range(seqs):
        x = heads_in[s].astype(F32)
        turned = x * cosines[s : s + 1, :] + pltpu.roll(x, HEAD_DIM // 2, 1) * sines[s : s + 1, :]
        turned = turned.astype(BF16)
        query = turned[:queries]
        rounded = turned.astype(F32)
        own_key = rounded[queries : queries + 1]
        own_value = x[queries + kv : queries + kv + 1]
        own_key = jnp.broadcast_to(own_key, (queries, HEAD_DIM))
        own_value = jnp.broadcast_to(own_value, (queries, HEAD_DIM))
        scores = None
        for h in range(kv):
            part = lax.dot_general(
                query,
                keys[s, :, h * HEAD_DIM : (h + 1) * HEAD_DIM],
                (((1,), (1,)), ((), ())),
                preferred_element_type=F32,
            )
            scores = part if h == 0 else jnp.where(wide_head == h, part, scores)
            if h:
                own_key = jnp.where(head == h, rounded[queries + h : queries + h + 1], own_key)
                at = queries + kv + h
                own_value = jnp.where(head == h, x[at : at + 1], own_value)
        scores = scores / root
        own = jnp.sum(rounded[:queries] * own_key, axis=-1, keepdims=True) / root
        visible = place < lengths[s]
        highest = jnp.maximum(
            jnp.max(jnp.where(visible, scores, -1e30), axis=-1, keepdims=True), own
        )
        grown = jnp.where(visible, jnp.exp(scores - highest), 0.0)
        own_grown = jnp.exp(own - highest)
        total = jnp.sum(grown, axis=-1, keepdims=True) + own_grown
        probs = (grown / total).astype(BF16)
        own_prob = (own_grown / total).astype(BF16).astype(F32)
        mixed = None
        for h in range(kv):
            part = dot(probs, values[s, :, h * HEAD_DIM : (h + 1) * HEAD_DIM])
            mixed = part if h == 0 else jnp.where(head == h, part, mixed)
        out[s] = (mixed + own_prob * own_value).astype(BF16)


def moe_kernel(mine, x, out_sum, gain, router, routes, up, down, part, hidden, moe_in, gate, acc):
    step = pl.program_id(0)

    @pl.when(step == 0)
    def _():
        summed = (x[...].astype(F32) + out_sum[...]).astype(BF16)
        hidden[...] = summed
        wide = summed.astype(F32)
        scale = lax.rsqrt(jnp.mean(wide * wide, axis=-1, keepdims=True) + norm_eps)
        normed = (wide * scale * gain[...]).astype(BF16)
        moe_in[...] = normed
        logits = dot(normed, router[...])
        lane = lax.broadcasted_iota(jnp.int32, logits.shape, 1).astype(F32)
        first = routes[:, 0:1].astype(F32)
        second = routes[:, 1:2].astype(F32)
        at_first = jnp.sum(jnp.where(lane == first, logits, 0.0), axis=-1, keepdims=True)
        at_second = jnp.sum(jnp.where(lane == second, logits, 0.0), axis=-1, keepdims=True)
        expert = mine[0].astype(F32)
        weight = jnp.where(first == expert, 1.0 / (1.0 + jnp.exp(at_second - at_first)), 0.0)
        weight += jnp.where(second == expert, 1.0 / (1.0 + jnp.exp(at_first - at_second)), 0.0)
        gate[...] = jnp.broadcast_to(weight, gate.shape)
        acc[...] = jnp.zeros_like(acc)

    lifted = dot(moe_in[...], up[...])
    active = (lifted / (1.0 + jnp.exp(-lifted))).astype(BF16)
    acc[...] += dot(active, down[...])

    @pl.when(step == pl.num_programs(0) - 1)
    def _():
        part[...] = (gate[:, 0:1] * acc[...]).astype(BF16)


def moe_call(mine, x, out_sum, gain, router, routes, up, down):
    rows, width = x.shape
    units = up.shape[1]
    tile = next((t for t in (512, 256, 128) if units % t == 0), units)
    whole = lambda a: pl.BlockSpec(a.shape, lambda i: (0,) * a.ndim)
    return pl.pallas_call(
        moe_kernel,
        grid=(units // tile,),
        in_specs=[
            pl.BlockSpec(memory_space=pltpu.SMEM),
            whole(x),
            whole(out_sum),
            whole(gain),
            whole(router),
            whole(routes),
            pl.BlockSpec((width, tile), lambda i: (0, i)),
            pl.BlockSpec((tile, width), lambda i: (i, 0)),
        ],
        out_specs=[pl.BlockSpec((rows, width), lambda i: (0, 0))] * 2,
        out_shape=[jax.ShapeDtypeStruct((rows, width), BF16)] * 2,
        scratch_shapes=[
            pltpu.VMEM((rows, width), BF16),
            pltpu.VMEM((rows, 128), F32),
            pltpu.VMEM((rows, width), F32),
        ],
        compiler_params=pltpu.CompilerParams(
            dimension_semantics=("arbitrary",), vmem_limit_bytes=40 * 1024 * 1024
        ),
        name="moe",
    )(mine, x, out_sum, gain, router, routes, up, down)


def qkv_kernel(x, gain, weight, out):
    wide = x[...].astype(F32)
    scale = lax.rsqrt(jnp.mean(wide * wide, axis=-1, keepdims=True) + norm_eps)
    out[...] = dot((wide * scale * gain[...]).astype(BF16), weight[...]).astype(BF16)


def per_device(
    tokens,
    lengths,
    routes,
    attn_gain,
    w_qkv,
    w_out,
    moe_gain,
    router,
    w_up,
    w_down,
    k_codes,
    k_scale,
    k_zero,
    v_codes,
    v_scale,
    v_zero,
):
    section = lax.axis_index("section")
    sections = lax.axis_size("section")
    index = lax.axis_index("expert")
    devs = lax.axis_size("expert")
    rows, width = tokens.shape
    mine = (index // (devs // EXPERTS)).astype(jnp.int32).reshape(1)
    router_wide = jnp.pad(router[0], ((0, 0), (0, 128 - EXPERTS)))
    sent = jnp.concatenate(
        [tokens, jnp.pad(routes[0].astype(BF16), ((0, 0), (0, 126)))], axis=1
    )
    got = gathered(sent, 0)
    x = got[:, :width]
    route_rows = got[:, width:]
    total_rows = x.shape[0]
    queries = w_out.shape[1] // HEAD_DIM
    frequency = jnp.power(rope_base, -2.0 * jnp.arange(HEAD_DIM // 2, dtype=F32) / HEAD_DIM)
    angles = lengths.astype(F32)[:, None] * frequency[None, :]
    cosine = jnp.cos(angles)
    sine = jnp.sin(angles)
    cosines = jnp.concatenate([cosine, cosine], axis=-1)
    sines = jnp.concatenate([-sine, sine], axis=-1)
    cache = jax.ShapeDtypeStruct((rows, k_codes.shape[2] * WORD, k_codes.shape[3]), BF16)
    keys, values = pl.pallas_call(dequant_kernel, out_shape=[cache, cache], name="dequant")(
        k_codes[0], k_scale[0], k_zero[0], v_codes[0], v_scale[0], v_zero[0]
    )
    row_owner = (jnp.arange(total_rows, dtype=jnp.int32) // rows)[:, None]
    kept = None
    for tick in range(sections):
        columns = pl.pallas_call(
            qkv_kernel,
            out_shape=jax.ShapeDtypeStruct((total_rows, w_qkv.shape[3]), BF16),
            name="qkv",
        )(x, attn_gain, w_qkv[0, 0])
        own = to_owners(columns, rows).reshape(rows, -1, HEAD_DIM)
        attended = pl.pallas_call(
            attention_kernel,
            in_specs=[pl.BlockSpec(memory_space=pltpu.SMEM)]
            + [pl.BlockSpec(memory_space=pltpu.VMEM)] * 5,
            out_shape=jax.ShapeDtypeStruct((rows, queries, HEAD_DIM), BF16),
            name="attention",
        )(lengths, own, cosines, sines, keys, values)
        mixed = gathered(attended.reshape(rows, -1), 0)
        out_part = dot(mixed, w_out[0])
        out_cols = (out_part + partner(out_part)).astype(BF16)
        out_sum = gathered(out_cols, 1).astype(F32)
        part, hidden = moe_call(
            mine, x, out_sum, moe_gain, router_wide, route_rows, w_up[0], w_down[0]
        )
        both = part.astype(F32) + partner(part).astype(F32)
        both = both + jnp.where(row_owner == index, hidden.astype(F32), 0.0)
        kept = both if kept is None else jnp.where(section == tick, both, kept)
        if tick + 1 < sections:
            x = next_section_sum(both.astype(BF16)).astype(BF16)
    result = summed_at_owners(row_block(kept, index, rows), kept.astype(BF16), rows)
    return result.astype(BF16).reshape(1, rows, width)


def solution(mesh):
    return jax.shard_map(
        per_device,
        mesh=mesh,
        in_specs=(
            P(("group", "expert"), None),
            P(("group", "expert")),
            P("section", ("group", "expert"), None),
            P("section", None),
            P("section", "tensor", None, "expert"),
            P("section", "tensor", "expert"),
            P("section", None),
            P("section", None, None),
            P("section", None, ("expert", "tensor")),
            P("section", ("expert", "tensor"), None),
            P("section", ("group", "expert"), None, "tensor"),
            P("section", ("group", "expert"), None, "tensor"),
            P("section", ("group", "expert"), None, "tensor"),
            P("section", ("group", "expert"), None, "tensor"),
            P("section", ("group", "expert"), "tensor", None),
            P("section", ("group", "expert"), "tensor", None),
        ),
        out_specs=P("section", ("group", "expert"), None),
        check_vma=False,
    )
```

```python
import functools
import math

import jax
import jax.numpy as jnp
from jax import lax
from jax.experimental import pallas as pl
from jax.experimental.pallas import tpu as pltpu
from jax.sharding import PartitionSpec as P

HEAD_DIM = 128
EXPERTS = 4
WORD = 16
rope_base = 1000000.0
norm_eps = 1e-05
FEW = 8
F32 = jnp.float32
BF16 = jnp.bfloat16


COVER = pl.CostEstimate(flops=8_000_000_000, bytes_accessed=30_000_000, transcendentals=0)
SMALL = pltpu.CompilerParams(vmem_limit_bytes=8 * 1024 * 1024)


def shifted(array, by):
    n = lax.axis_size("expert")
    return lax.ppermute(array, "expert", [(i, (i + by) % n) for i in range(n)])


def arrange(pieces, index, axis):
    return jnp.concatenate([placed(pieces, index, j) for j in range(len(pieces))], axis=axis)


def gathered_pieces(array, axis):
    n = lax.axis_size("expert")
    if n > FEW:
        return [lax.all_gather(array, "expert", axis=axis, tiled=True)]
    return [array] + [shifted(array, k) for k in range(1, n)]


def placed(pieces, index, j):
    n = len(pieces)
    chunk = pieces[0]
    for k in range(1, n):
        chunk = jnp.where((index + (n - k)) % n == j, pieces[k], chunk)
    return chunk


def row_block(array, block, rows):
    return lax.dynamic_slice_in_dim(array, block * rows, rows, 0)


def to_owners(blocks):
    n = lax.axis_size("expert")
    if n > FEW:
        return [
            lax.all_to_all(blocks[0], "expert", split_axis=0, concat_axis=1, tiled=True)
        ]
    return [blocks[0]] + [shifted(blocks[k], k) for k in range(1, n)]


def summed_at_owners(own, array, rows):
    n = lax.axis_size("expert")
    index = lax.axis_index("expert")
    if n > FEW:
        got = lax.all_to_all(
            array.reshape(n, rows, -1), "expert", split_axis=0, concat_axis=0, tiled=True
        ).astype(F32)
        return jnp.sum(jnp.where(jnp.arange(n)[:, None, None] == index, own[None], got), axis=0)
    total = own
    for k in range(1, n):
        total = total + shifted(row_block(array, (index + k) % n, rows), k).astype(F32)
    return total


def next_section_parts(array):
    n = lax.axis_size("expert")
    sections = lax.axis_size("section")
    if n > FEW:
        moved = lax.ppermute(array, "section", [(s, s + 1) for s in range(sections - 1)])
        return [lax.psum(moved.astype(F32), "expert").astype(BF16)]
    parts = []
    for k in range(n):
        pairs = [
            (e * sections + s, ((e + k) % n) * sections + s + 1)
            for e in range(n)
            for s in range(sections - 1)
        ]
        parts.append(lax.ppermute(array, ("expert", "section"), pairs))
    return parts


def partner(array):
    n = lax.axis_size("tensor")
    return lax.ppermute(array, "tensor", [(i, n - 1 - i) for i in range(n)])


def dot(a, b):
    return jnp.dot(a, b, preferred_element_type=F32)


def dequant_kernel(kc, ks, kz, vc, vs, vz, keys, values):
    seqs, words, channels = kc.shape
    positions = words * WORD
    key_groups = ks.shape[1]
    value_groups = vs.shape[1]
    row = lax.broadcasted_iota(jnp.int32, (positions, positions), 0)
    col = lax.broadcasted_iota(jnp.int32, (positions, positions), 1)
    order = jnp.where(col == (row % words) * WORD + row // words, 1.0, 0.0).astype(BF16)
    group_row = lax.broadcasted_iota(jnp.int32, (value_groups, channels), 0)
    group_col = lax.broadcasted_iota(jnp.int32, (value_groups, channels), 1)
    spread = jnp.where(group_row == group_col // (channels // value_groups), 1.0, 0.0).astype(BF16)
    word_row = lax.broadcasted_iota(jnp.int32, (words, key_groups), 0)
    word_col = lax.broadcasted_iota(jnp.int32, (words, key_groups), 1)
    repeat = jnp.where(word_row // (words // key_groups) == word_col, 1.0, 0.0).astype(BF16)

    def expand(table):
        wide = lax.dot_general(table, spread, (((0,), (0,)), ((), ())), preferred_element_type=F32)
        return dot(order, wide.astype(BF16))

    for s in range(seqs):
        key_scale = dot(repeat, ks[s])
        key_zero = dot(repeat, kz[s])
        value_scale = expand(vs[s])
        value_zero = expand(vz[s])
        for i in range(WORD):
            at = slice(i * words, (i + 1) * words)
            code = ((kc[s] >> (2 * i)) & 3).astype(F32)
            keys[s, at, :] = (code * key_scale + key_zero).astype(BF16)
            code = ((vc[s] >> (2 * i)) & 3).astype(F32)
            values[s, at, :] = (code * value_scale[at] + value_zero[at]).astype(BF16)


def attention_kernel(index, lengths, *refs):
    *pieces, cosines, sines, keys, values, out = refs
    seqs, positions, channels = keys.shape
    kv = channels // HEAD_DIM
    queries = out.shape[1] // HEAD_DIM
    joined = arrange([piece[...].astype(F32) for piece in pieces], index[0], 1)
    finished = []
    ratio = queries // kv
    words = positions // WORD
    place = lax.broadcasted_iota(jnp.int32, (queries, positions), 1)
    place = (place % words) * WORD + place // words
    head = lax.broadcasted_iota(jnp.int32, (queries, HEAD_DIM), 0) // ratio
    wide_head = lax.broadcasted_iota(jnp.int32, (queries, positions), 0) // ratio
    root = math.sqrt(HEAD_DIM)
    for s in range(seqs):
        x = jnp.concatenate(
            [
                joined[s : s + 1, h * HEAD_DIM : (h + 1) * HEAD_DIM]
                for h in range(queries + 2 * kv)
            ],
            axis=0,
        )
        turned = x * cosines[s : s + 1, :] + pltpu.roll(x, HEAD_DIM // 2, 1) * sines[s : s + 1, :]
        turned = turned.astype(BF16)
        query = turned[:queries]
        rounded = turned.astype(F32)
        own_key = rounded[queries : queries + 1]
        own_value = x[queries + kv : queries + kv + 1]
        own_key = jnp.broadcast_to(own_key, (queries, HEAD_DIM))
        own_value = jnp.broadcast_to(own_value, (queries, HEAD_DIM))
        scores = None
        for h in range(kv):
            part = lax.dot_general(
                query,
                keys[s, :, h * HEAD_DIM : (h + 1) * HEAD_DIM],
                (((1,), (1,)), ((), ())),
                preferred_element_type=F32,
            )
            scores = part if h == 0 else jnp.where(wide_head == h, part, scores)
            if h:
                own_key = jnp.where(head == h, rounded[queries + h : queries + h + 1], own_key)
                at = queries + kv + h
                own_value = jnp.where(head == h, x[at : at + 1], own_value)
        scores = scores / root
        own = jnp.sum(rounded[:queries] * own_key, axis=-1, keepdims=True) / root
        visible = place < lengths[s]
        highest = jnp.maximum(
            jnp.max(jnp.where(visible, scores, -1e30), axis=-1, keepdims=True), own
        )
        grown = jnp.where(visible, jnp.exp(scores - highest), 0.0)
        own_grown = jnp.exp(own - highest)
        total = jnp.sum(grown, axis=-1, keepdims=True) + own_grown
        probs = (grown / total).astype(BF16)
        own_prob = (own_grown / total).astype(BF16).astype(F32)
        mixed = None
        for h in range(kv):
            part = dot(probs, values[s, :, h * HEAD_DIM : (h + 1) * HEAD_DIM])
            mixed = part if h == 0 else jnp.where(head == h, part, mixed)
        mixed = mixed + own_prob * own_value
        finished.append(jnp.concatenate([mixed[h : h + 1] for h in range(queries)], axis=1))
    out[...] = jnp.concatenate(finished, axis=0).astype(BF16)


def moe_kernel(mine, index, x, gain, router, routes, up, down, *refs):
    *pieces, part, hidden = refs
    out_sum = arrange([piece[...].astype(F32) for piece in pieces], index[0], 1)
    summed = (x[...].astype(F32) + out_sum).astype(BF16)
    hidden[...] = summed
    wide = summed.astype(F32)
    scale = lax.rsqrt(jnp.mean(wide * wide, axis=-1, keepdims=True) + norm_eps)
    normed = (wide * scale * gain[...]).astype(BF16)
    rounded = normed.astype(F32)
    first = routes[:, 0:1].astype(F32)
    second = routes[:, 1:2].astype(F32)
    at_first = jnp.zeros_like(first)
    at_second = jnp.zeros_like(second)
    for j in range(EXPERTS):
        logit = jnp.sum(rounded * router[j : j + 1, :].astype(F32), axis=-1, keepdims=True)
        at_first += jnp.where(first == float(j), logit, 0.0)
        at_second += jnp.where(second == float(j), logit, 0.0)
    expert = mine[0].astype(F32)
    gate = jnp.where(first == expert, 1.0 / (1.0 + jnp.exp(at_second - at_first)), 0.0)
    gate += jnp.where(second == expert, 1.0 / (1.0 + jnp.exp(at_first - at_second)), 0.0)
    units = up.shape[1]
    tile = next((t for t in (512, 256, 128) if units % t == 0), units)
    total = None
    for start in range(0, units, tile):
        lifted = dot(normed, up[:, start : start + tile])
        active = (lifted / (1.0 + jnp.exp(-lifted))).astype(BF16)
        lowered = dot(active, down[start : start + tile, :])
        total = lowered if total is None else total + lowered
    part[...] = (gate * total).astype(BF16)


IN_SMEM = pl.BlockSpec(memory_space=pltpu.SMEM)
IN_VMEM = pl.BlockSpec(memory_space=pltpu.VMEM)


def moe_call(mine, index, x, gain, router, routes, up, down, pieces):
    return pl.pallas_call(
        moe_kernel,
        in_specs=[IN_SMEM] * 2 + [IN_VMEM] * (6 + len(pieces)),
        out_shape=[jax.ShapeDtypeStruct(x.shape, BF16)] * 2,
        compiler_params=SMALL,
        name="moe",
    )(mine, index, x, gain, router, routes, up, down, *pieces)


def out_kernel(index, weight, *refs):
    *pieces, out, scratch = refs
    rows = pieces[0].shape[0]
    loaded = [piece[...].astype(F32) for piece in pieces]
    for j in range(len(pieces)):
        scratch[j * rows : (j + 1) * rows, :] = placed(loaded, index[0], j)
    out[...] = dot(scratch[...].astype(BF16), weight[...])


def project(rows_f32, gain, weight, index, outs):
    scale = lax.rsqrt(jnp.mean(rows_f32 * rows_f32, axis=-1, keepdims=True) + norm_eps)
    columns = dot((rows_f32 * scale * gain[...]).astype(BF16), weight[...])
    n = len(outs)
    rows = outs[0].shape[0]
    for k in range(n):
        block = columns[:rows]
        for j in range(1, n):
            block = jnp.where((index[0] + k) % n == j, columns[j * rows : (j + 1) * rows], block)
        outs[k][...] = block.astype(BF16)


def first_kernel(count, index, gain, weight, *refs):
    pieces, (x, routes, *outs), scratch = refs[:count], refs[count:-1], refs[-1]
    rows = pieces[0].shape[0]
    width = x.shape[1]
    loaded = [piece[...].astype(F32) for piece in pieces]
    for j in range(count):
        scratch[j * rows : (j + 1) * rows, :] = placed(loaded, index[0], j)
    wide = scratch[:, :width]
    x[...] = wide.astype(BF16)
    routes[...] = scratch[:, width:].astype(BF16)
    project(wide, gain, weight, index, outs)


def later_kernel(count, index, gain, weight, *refs):
    parts, (x, *outs) = refs[:count], refs[count:]
    total = parts[0][...].astype(F32)
    for part in parts[1:]:
        total = total + part[...].astype(F32)
    x[...] = total.astype(BF16)
    project(x[...].astype(F32), gain, weight, index, outs)


def per_device(
    tokens,
    lengths,
    routes,
    attn_gain,
    w_qkv,
    w_out,
    moe_gain,
    router,
    w_up,
    w_down,
    k_codes,
    k_scale,
    k_zero,
    v_codes,
    v_scale,
    v_zero,
):
    section = lax.axis_index("section")
    sections = lax.axis_size("section")
    index = lax.axis_index("expert")
    devs = lax.axis_size("expert")
    rows, width = tokens.shape
    mine = (index // (devs // EXPERTS)).astype(jnp.int32).reshape(1)
    spot = index.astype(jnp.int32).reshape(1)
    router_rows = jnp.swapaxes(router[0], 0, 1)
    few = devs <= FEW
    sent = jnp.concatenate([tokens, jnp.pad(routes[0].astype(BF16), ((0, 0), (0, 126)))], axis=1)
    sources = gathered_pieces(sent, 0)
    total_rows = rows * devs
    queries = w_out.shape[1] // HEAD_DIM
    x_shape = jax.ShapeDtypeStruct((total_rows, width), BF16)
    block_shapes = [
        jax.ShapeDtypeStruct((rows if few else total_rows, w_qkv.shape[3]), BF16)
    ] * (devs if few else 1)
    frequency = jnp.power(rope_base, -2.0 * jnp.arange(HEAD_DIM // 2, dtype=F32) / HEAD_DIM)
    angles = lengths.astype(F32)[:, None] * frequency[None, :]
    cosine = jnp.cos(angles)
    sine = jnp.sin(angles)
    cosines = jnp.concatenate([cosine, cosine], axis=-1)
    sines = jnp.concatenate([-sine, sine], axis=-1)
    cache = jax.ShapeDtypeStruct((rows, k_codes.shape[2] * WORD, k_codes.shape[3]), BF16)
    keys, values = pl.pallas_call(dequant_kernel, out_shape=[cache, cache], name="dequant", compiler_params=SMALL, cost_estimate=COVER)(
        k_codes[0], k_scale[0], k_zero[0], v_codes[0], v_scale[0], v_zero[0]
    )
    row_owner = (jnp.arange(total_rows, dtype=jnp.int32) // rows)[:, None]
    kept = None
    for tick in range(sections):
        count = len(sources)
        specs = [IN_SMEM] + [IN_VMEM] * (2 + count)
        if tick == 0:
            x, route_rows, *blocks = pl.pallas_call(
                functools.partial(first_kernel, count),
                in_specs=specs,
                out_shape=[x_shape, jax.ShapeDtypeStruct((total_rows, 128), BF16)] + block_shapes,
                scratch_shapes=[pltpu.VMEM((total_rows, width + 128), F32)],
                compiler_params=SMALL,
                cost_estimate=COVER,
                name="first_qkv",
            )(spot, attn_gain, w_qkv[0, 0], *sources)
        else:
            x, *blocks = pl.pallas_call(
                functools.partial(later_kernel, count),
                in_specs=specs,
                out_shape=[x_shape] + block_shapes,
                compiler_params=SMALL,
                cost_estimate=COVER,
                name="later_qkv",
            )(spot, attn_gain, w_qkv[0, 0], *sources)
        own = to_owners(blocks)
        attended = pl.pallas_call(
            attention_kernel,
            in_specs=[IN_SMEM] * 2 + [IN_VMEM] * (4 + len(own)),
            out_shape=jax.ShapeDtypeStruct((rows, queries * HEAD_DIM), BF16),
            compiler_params=SMALL,
            cost_estimate=COVER,
            name="attention",
        )(spot, lengths, *own, cosines, sines, keys, values)
        pieces = gathered_pieces(attended, 0)
        out_part = pl.pallas_call(
            out_kernel,
            in_specs=[IN_SMEM] + [IN_VMEM] * (1 + len(pieces)),
            out_shape=jax.ShapeDtypeStruct((total_rows, w_out.shape[2]), F32),
            scratch_shapes=[pltpu.VMEM((total_rows, w_out.shape[1]), F32)],
            compiler_params=SMALL,
            cost_estimate=COVER,
            name="out_projection",
        )(spot, w_out[0], *pieces)
        out_cols = (out_part + partner(out_part)).astype(BF16)
        part, hidden = moe_call(
            mine,
            spot,
            x,
            moe_gain,
            router_rows,
            route_rows,
            w_up[0],
            w_down[0],
            gathered_pieces(out_cols, 1),
        )
        both = part.astype(F32) + partner(part).astype(F32)
        both = both + jnp.where(row_owner == index, hidden.astype(F32), 0.0)
        kept = both if kept is None else jnp.where(section == tick, both, kept)
        if tick + 1 < sections:
            sources = next_section_parts(both.astype(BF16))
    result = summed_at_owners(row_block(kept, index, rows), kept.astype(BF16), rows)
    return result.astype(BF16).reshape(1, rows, width)


def solution(mesh):
    return jax.shard_map(
        per_device,
        mesh=mesh,
        in_specs=(
            P(("group", "expert"), None),
            P(("group", "expert")),
            P("section", ("group", "expert"), None),
            P("section", None),
            P("section", "tensor", None, "expert"),
            P("section", "tensor", "expert"),
            P("section", None),
            P("section", None, None),
            P("section", None, ("expert", "tensor")),
            P("section", ("expert", "tensor"), None),
            P("section", ("group", "expert"), None, "tensor"),
            P("section", ("group", "expert"), None, "tensor"),
            P("section", ("group", "expert"), None, "tensor"),
            P("section", ("group", "expert"), None, "tensor"),
            P("section", ("group", "expert"), "tensor", None),
            P("section", ("group", "expert"), "tensor", None),
        ),
        out_specs=P("section", ("group", "expert"), None),
        check_vma=False,
    )
```

```python
import functools
import math

import jax
import jax.numpy as jnp
from jax import lax
from jax.experimental import pallas as pl
from jax.experimental.pallas import tpu as pltpu
from jax.sharding import PartitionSpec as P

HEAD_DIM = 128
EXPERTS = 4
WORD = 16
rope_base = 1000000.0
norm_eps = 1e-05
FEW = 8
F32 = jnp.float32
BF16 = jnp.bfloat16


COVER = pl.CostEstimate(flops=8_000_000_000, bytes_accessed=30_000_000, transcendentals=0)
SMALL = pltpu.CompilerParams(vmem_limit_bytes=8 * 1024 * 1024)


def shifted(array, by):
    n = lax.axis_size("expert")
    return lax.ppermute(array, "expert", [(i, (i + by) % n) for i in range(n)])


def arrange(pieces, index, axis):
    return jnp.concatenate([placed(pieces, index, j) for j in range(len(pieces))], axis=axis)


def gathered_pieces(array, axis):
    n = lax.axis_size("expert")
    if n > FEW:
        return [lax.all_gather(array, "expert", axis=axis, tiled=True)]
    return [array] + [shifted(array, k) for k in range(1, n)]


def placed(pieces, index, j):
    n = len(pieces)
    chunk = pieces[0]
    for k in range(1, n):
        chunk = jnp.where((index + (n - k)) % n == j, pieces[k], chunk)
    return chunk


def row_block(array, block, rows):
    return lax.dynamic_slice_in_dim(array, block * rows, rows, 0)


def to_owners(blocks):
    n = lax.axis_size("expert")
    if n > FEW:
        return [
            lax.all_to_all(blocks[0], "expert", split_axis=0, concat_axis=1, tiled=True)
        ]
    return [blocks[0]] + [shifted(blocks[k], k) for k in range(1, n)]


def summed_at_owners(own, array, rows):
    n = lax.axis_size("expert")
    index = lax.axis_index("expert")
    if n > FEW:
        got = lax.all_to_all(
            array.reshape(n, rows, -1), "expert", split_axis=0, concat_axis=0, tiled=True
        ).astype(F32)
        return jnp.sum(jnp.where(jnp.arange(n)[:, None, None] == index, own[None], got), axis=0)
    total = own
    for k in range(1, n):
        total = total + shifted(row_block(array, (index + k) % n, rows), k).astype(F32)
    return total


def next_section_parts(array):
    n = lax.axis_size("expert")
    sections = lax.axis_size("section")
    if n > FEW:
        moved = lax.ppermute(array, "section", [(s, s + 1) for s in range(sections - 1)])
        return [lax.psum(moved.astype(F32), "expert").astype(BF16)]
    cores = lax.axis_size("tensor")
    total = None
    for k in range(0, n, cores):
        pairs = [
            (
                (e * cores + t) * sections + s,
                ((e + k + t) % n * cores + t) * sections + s + 1,
            )
            for e in range(n)
            for t in range(cores)
            for s in range(sections - 1)
        ]
        part = lax.ppermute(array, ("expert", "tensor", "section"), pairs).astype(F32)
        total = part if total is None else total + part
    total = total.astype(BF16)
    return [total, partner(total)]


def partner(array):
    n = lax.axis_size("tensor")
    return lax.ppermute(array, "tensor", [(i, n - 1 - i) for i in range(n)])


def dot(a, b):
    return jnp.dot(a, b, preferred_element_type=F32)


def dequant_kernel(*refs):
    stored, (_, keys, values), loaded, sems = refs[:6], refs[6:9], refs[9:15], refs[15]
    copies = [pltpu.make_async_copy(stored[i], loaded[i], sems.at[i]) for i in range(6)]
    for copy in copies:
        copy.start()
    for copy in copies:
        copy.wait()
    kc, ks, kz, vc, vs, vz = loaded
    seqs, words, channels = kc.shape
    positions = words * WORD
    key_groups = ks.shape[1]
    value_groups = vs.shape[1]
    row = lax.broadcasted_iota(jnp.int32, (positions, positions), 0)
    col = lax.broadcasted_iota(jnp.int32, (positions, positions), 1)
    order = jnp.where(col == (row % words) * WORD + row // words, 1.0, 0.0).astype(BF16)
    group_row = lax.broadcasted_iota(jnp.int32, (value_groups, channels), 0)
    group_col = lax.broadcasted_iota(jnp.int32, (value_groups, channels), 1)
    spread = jnp.where(group_row == group_col // (channels // value_groups), 1.0, 0.0).astype(BF16)
    word_row = lax.broadcasted_iota(jnp.int32, (words, key_groups), 0)
    word_col = lax.broadcasted_iota(jnp.int32, (words, key_groups), 1)
    repeat = jnp.where(word_row // (words // key_groups) == word_col, 1.0, 0.0).astype(BF16)

    def expand(table):
        wide = lax.dot_general(table, spread, (((0,), (0,)), ((), ())), preferred_element_type=F32)
        return dot(order, wide.astype(BF16))

    for s in range(seqs):
        key_scale = dot(repeat, ks[s])
        key_zero = dot(repeat, kz[s])
        value_scale = expand(vs[s])
        value_zero = expand(vz[s])
        for i in range(WORD):
            at = slice(i * words, (i + 1) * words)
            code = ((kc[s] >> (2 * i)) & 3).astype(F32)
            keys[s, at, :] = (code * key_scale + key_zero).astype(BF16)
            code = ((vc[s] >> (2 * i)) & 3).astype(F32)
            values[s, at, :] = (code * value_scale[at] + value_zero[at]).astype(BF16)


def attention_kernel(index, lengths, *refs):
    *pieces, cosines, sines, keys, values, out = refs
    seqs, positions, channels = keys.shape
    kv = channels // HEAD_DIM
    queries = out.shape[1] // HEAD_DIM
    joined = arrange([piece[...].astype(F32) for piece in pieces], index[0], 1)
    finished = []
    ratio = queries // kv
    words = positions // WORD
    place = lax.broadcasted_iota(jnp.int32, (queries, positions), 1)
    place = (place % words) * WORD + place // words
    head = lax.broadcasted_iota(jnp.int32, (queries, HEAD_DIM), 0) // ratio
    wide_head = lax.broadcasted_iota(jnp.int32, (queries, positions), 0) // ratio
    root = math.sqrt(HEAD_DIM)
    for s in range(seqs):
        x = jnp.concatenate(
            [
                joined[s : s + 1, h * HEAD_DIM : (h + 1) * HEAD_DIM]
                for h in range(queries + 2 * kv)
            ],
            axis=0,
        )
        turned = x * cosines[s : s + 1, :] + pltpu.roll(x, HEAD_DIM // 2, 1) * sines[s : s + 1, :]
        turned = turned.astype(BF16)
        query = turned[:queries]
        rounded = turned.astype(F32)
        own_key = rounded[queries : queries + 1]
        own_value = x[queries + kv : queries + kv + 1]
        own_key = jnp.broadcast_to(own_key, (queries, HEAD_DIM))
        own_value = jnp.broadcast_to(own_value, (queries, HEAD_DIM))
        scores = None
        for h in range(kv):
            part = lax.dot_general(
                query,
                keys[s, :, h * HEAD_DIM : (h + 1) * HEAD_DIM],
                (((1,), (1,)), ((), ())),
                preferred_element_type=F32,
            )
            scores = part if h == 0 else jnp.where(wide_head == h, part, scores)
            if h:
                own_key = jnp.where(head == h, rounded[queries + h : queries + h + 1], own_key)
                at = queries + kv + h
                own_value = jnp.where(head == h, x[at : at + 1], own_value)
        scores = scores / root
        own = jnp.sum(rounded[:queries] * own_key, axis=-1, keepdims=True) / root
        visible = place < lengths[s]
        highest = jnp.maximum(
            jnp.max(jnp.where(visible, scores, -1e30), axis=-1, keepdims=True), own
        )
        grown = jnp.where(visible, jnp.exp(scores - highest), 0.0)
        own_grown = jnp.exp(own - highest)
        total = jnp.sum(grown, axis=-1, keepdims=True) + own_grown
        probs = (grown / total).astype(BF16)
        own_prob = (own_grown / total).astype(BF16).astype(F32)
        mixed = None
        for h in range(kv):
            part = dot(probs, values[s, :, h * HEAD_DIM : (h + 1) * HEAD_DIM])
            mixed = part if h == 0 else jnp.where(head == h, part, mixed)
        mixed = mixed + own_prob * own_value
        finished.append(jnp.concatenate([mixed[h : h + 1] for h in range(queries)], axis=1))
    out[...] = jnp.concatenate(finished, axis=0).astype(BF16)


def moe_kernel(mine, index, x, gain, router, routes, up, down, *refs):
    *pieces, part, hidden = refs
    out_sum = arrange([piece[...].astype(F32) for piece in pieces], index[0], 1)
    summed = (x[...].astype(F32) + out_sum).astype(BF16)
    hidden[...] = summed
    wide = summed.astype(F32)
    scale = lax.rsqrt(jnp.mean(wide * wide, axis=-1, keepdims=True) + norm_eps)
    normed = (wide * scale * gain[...]).astype(BF16)
    rounded = normed.astype(F32)
    first = routes[:, 0:1].astype(F32)
    second = routes[:, 1:2].astype(F32)
    at_first = jnp.zeros_like(first)
    at_second = jnp.zeros_like(second)
    for j in range(EXPERTS):
        logit = jnp.sum(rounded * router[j : j + 1, :].astype(F32), axis=-1, keepdims=True)
        at_first += jnp.where(first == float(j), logit, 0.0)
        at_second += jnp.where(second == float(j), logit, 0.0)
    expert = mine[0].astype(F32)
    gate = jnp.where(first == expert, 1.0 / (1.0 + jnp.exp(at_second - at_first)), 0.0)
    gate += jnp.where(second == expert, 1.0 / (1.0 + jnp.exp(at_first - at_second)), 0.0)
    units = up.shape[1]
    tile = next((t for t in (512, 256, 128) if units % t == 0), units)
    total = None
    for start in range(0, units, tile):
        lifted = dot(normed, up[:, start : start + tile])
        active = (lifted / (1.0 + jnp.exp(-lifted))).astype(BF16)
        lowered = dot(active, down[start : start + tile, :])
        total = lowered if total is None else total + lowered
    part[...] = (gate * total).astype(BF16)


IN_SMEM = pl.BlockSpec(memory_space=pltpu.SMEM)
IN_VMEM = pl.BlockSpec(memory_space=pltpu.VMEM)


def moe_call(mine, index, x, gain, router, routes, up, down, pieces):
    return pl.pallas_call(
        moe_kernel,
        in_specs=[IN_SMEM] * 2 + [IN_VMEM] * (6 + len(pieces)),
        out_shape=[jax.ShapeDtypeStruct(x.shape, BF16)] * 2,
        compiler_params=SMALL,
        name="moe",
    )(mine, index, x, gain, router, routes, up, down, *pieces)


def out_kernel(index, weight, *refs):
    *pieces, out, scratch = refs
    rows = pieces[0].shape[0]
    loaded = [piece[...].astype(F32) for piece in pieces]
    for j in range(len(pieces)):
        scratch[j * rows : (j + 1) * rows, :] = placed(loaded, index[0], j)
    out[...] = dot(scratch[...].astype(BF16), weight[...])


def project(rows_f32, gain, weight, index, outs):
    scale = lax.rsqrt(jnp.mean(rows_f32 * rows_f32, axis=-1, keepdims=True) + norm_eps)
    columns = dot((rows_f32 * scale * gain[...]).astype(BF16), weight[...])
    n = len(outs)
    rows = outs[0].shape[0]
    for k in range(n):
        block = columns[:rows]
        for j in range(1, n):
            block = jnp.where((index[0] + k) % n == j, columns[j * rows : (j + 1) * rows], block)
        outs[k][...] = block.astype(BF16)


def first_kernel(count, index, gain, weight, *refs):
    pieces, (x, routes, *outs), scratch = refs[:count], refs[count:-1], refs[-1]
    rows = pieces[0].shape[0]
    width = x.shape[1]
    loaded = [piece[...].astype(F32) for piece in pieces]
    for j in range(count):
        scratch[j * rows : (j + 1) * rows, :] = placed(loaded, index[0], j)
    wide = scratch[:, :width]
    x[...] = wide.astype(BF16)
    routes[...] = scratch[:, width:].astype(BF16)
    project(wide, gain, weight, index, outs)


def later_kernel(count, index, gain, weight, *refs):
    parts, (x, *outs) = refs[:count], refs[count:]
    total = parts[0][...].astype(F32)
    for part in parts[1:]:
        total = total + part[...].astype(F32)
    x[...] = total.astype(BF16)
    project(x[...].astype(F32), gain, weight, index, outs)


def per_device(
    tokens,
    lengths,
    routes,
    attn_gain,
    w_qkv,
    w_out,
    moe_gain,
    router,
    w_up,
    w_down,
    k_codes,
    k_scale,
    k_zero,
    v_codes,
    v_scale,
    v_zero,
):
    section = lax.axis_index("section")
    sections = lax.axis_size("section")
    index = lax.axis_index("expert")
    devs = lax.axis_size("expert")
    rows, width = tokens.shape
    mine = (index // (devs // EXPERTS)).astype(jnp.int32).reshape(1)
    spot = index.astype(jnp.int32).reshape(1)
    router_rows = jnp.swapaxes(router[0], 0, 1)
    few = devs <= FEW
    sent = jnp.concatenate([tokens, jnp.pad(routes[0].astype(BF16), ((0, 0), (0, 126)))], axis=1)
    sources = gathered_pieces(sent, 0)
    total_rows = rows * devs
    queries = w_out.shape[1] // HEAD_DIM
    x_shape = jax.ShapeDtypeStruct((total_rows, width), BF16)
    block_shapes = [
        jax.ShapeDtypeStruct((rows if few else total_rows, w_qkv.shape[3]), BF16)
    ] * (devs if few else 1)
    frequency = jnp.power(rope_base, -2.0 * jnp.arange(HEAD_DIM // 2, dtype=F32) / HEAD_DIM)
    angles = lengths.astype(F32)[:, None] * frequency[None, :]
    cosine = jnp.cos(angles)
    sine = jnp.sin(angles)
    cosines = jnp.concatenate([cosine, cosine], axis=-1)
    sines = jnp.concatenate([-sine, sine], axis=-1)
    cache = jax.ShapeDtypeStruct((rows, k_codes.shape[2] * WORD, k_codes.shape[3]), BF16)
    tables = [k_codes[0], k_scale[0], k_zero[0], v_codes[0], v_scale[0], v_zero[0]]
    row_owner = (jnp.arange(total_rows, dtype=jnp.int32) // rows)[:, None]
    kept = None
    for tick in range(sections):
        count = len(sources)
        specs = [IN_SMEM] + [IN_VMEM] * (2 + count)
        if tick == 0:
            x, route_rows, *blocks = pl.pallas_call(
                functools.partial(first_kernel, count),
                in_specs=specs,
                out_shape=[x_shape, jax.ShapeDtypeStruct((total_rows, 128), BF16)] + block_shapes,
                scratch_shapes=[pltpu.VMEM((total_rows, width + 128), F32)],
                compiler_params=SMALL,
                cost_estimate=COVER,
                name="first_qkv",
            )(spot, attn_gain, w_qkv[0, 0], *sources)
            keys, values = pl.pallas_call(
                dequant_kernel,
                in_specs=[pl.BlockSpec(memory_space=pl.ANY)] * 6 + [IN_VMEM],
                out_shape=[cache, cache],
                scratch_shapes=[pltpu.VMEM(t.shape, t.dtype) for t in tables]
                + [pltpu.SemaphoreType.DMA((6,))],
                compiler_params=SMALL,
                cost_estimate=COVER,
                name="dequant",
            )(*tables, blocks[0])
        else:
            x, *blocks = pl.pallas_call(
                functools.partial(later_kernel, count),
                in_specs=specs,
                out_shape=[x_shape] + block_shapes,
                compiler_params=SMALL,
                cost_estimate=COVER,
                name="later_qkv",
            )(spot, attn_gain, w_qkv[0, 0], *sources)
        own = to_owners(blocks)
        attended = pl.pallas_call(
            attention_kernel,
            in_specs=[IN_SMEM] * 2 + [IN_VMEM] * (4 + len(own)),
            out_shape=jax.ShapeDtypeStruct((rows, queries * HEAD_DIM), BF16),
            compiler_params=SMALL,
            cost_estimate=COVER,
            name="attention",
        )(spot, lengths, *own, cosines, sines, keys, values)
        pieces = gathered_pieces(attended, 0)
        out_part = pl.pallas_call(
            out_kernel,
            in_specs=[IN_SMEM] + [IN_VMEM] * (1 + len(pieces)),
            out_shape=jax.ShapeDtypeStruct((total_rows, w_out.shape[2]), F32),
            scratch_shapes=[pltpu.VMEM((total_rows, w_out.shape[1]), F32)],
            compiler_params=SMALL,
            cost_estimate=COVER,
            name="out_projection",
        )(spot, w_out[0], *pieces)
        out_cols = (out_part + partner(out_part)).astype(BF16)
        part, hidden = moe_call(
            mine,
            spot,
            x,
            moe_gain,
            router_rows,
            route_rows,
            w_up[0],
            w_down[0],
            gathered_pieces(out_cols, 1),
        )
        both = part.astype(F32) + partner(part).astype(F32)
        both = both + jnp.where(row_owner == index, hidden.astype(F32), 0.0)
        kept = both if kept is None else jnp.where(section == tick, both, kept)
        if tick + 1 < sections:
            sources = next_section_parts(both.astype(BF16))
    result = summed_at_owners(row_block(kept, index, rows), kept.astype(BF16), rows)
    return result.astype(BF16).reshape(1, rows, width)


def solution(mesh):
    return jax.shard_map(
        per_device,
        mesh=mesh,
        in_specs=(
            P(("group", "expert"), None),
            P(("group", "expert")),
            P("section", ("group", "expert"), None),
            P("section", None),
            P("section", "tensor", None, "expert"),
            P("section", "tensor", "expert"),
            P("section", None),
            P("section", None, None),
            P("section", None, ("expert", "tensor")),
            P("section", ("expert", "tensor"), None),
            P("section", ("group", "expert"), None, "tensor"),
            P("section", ("group", "expert"), None, "tensor"),
            P("section", ("group", "expert"), None, "tensor"),
            P("section", ("group", "expert"), None, "tensor"),
            P("section", ("group", "expert"), "tensor", None),
            P("section", ("group", "expert"), "tensor", None),
        ),
        out_specs=P("section", ("group", "expert"), None),
        check_vma=False,
    )
```
